32 devices in a mesh: gx: 2 (over core), gy: 4 (over y, x), gz: 4 (over z).
Axes of the slice: x: 2, y: 2, z: 4, core: 2. Of those that a mesh axis runs over, the one named last changes fastest.
Arguments:
- sources: float32 [1, 32, 64, 512], P(None, 'gx', 'gy', 'gz'), may hold values from -6 to 6
- stiffness: float32 [32, 64, 512], P('gx', 'gy', 'gz'), may hold values from 0.5 to 2
- coarse_inverse: float32 [256, 256], P(('gx', 'gy', 'gz')), may hold values from -6 to 6
Outputs:
- pressure: float32 [1, 32, 64, 512], P(None, 'gx', 'gy', 'gz')
The draws below stay inside these ranges and needn't reach their ends.
All inputs are finite; a program needn't handle non-finite values.
Results may differ from the reference program's by a relative error of at most 0.0001.
Values sent between devices are 32-bit elements; how exact they have to be, the bound alone decides.
A program may use at most 64 MiB of HBM per device.

```python
import math
import jax
import jax.numpy as jnp
from jax import lax

SYSTEMS = 1
CX = 16
CY = 16
CZ = 128
NX = 32
NY = 64
NZ = 512
NC = 256
N_GX = 2
N_GY = 4
N_GZ = 4


def level_of(own_key, shape, cuts, smallest, largest):
    loudness = 1.0
    for dim, shards_of in cuts:
        steps = jax.random.uniform(jax.random.fold_in(jax.random.fold_in(own_key, 6), dim), (shards_of,), jnp.float32, smallest / len(cuts), largest / len(cuts))
        loudness = loudness * jnp.repeat(jnp.exp(steps), shape[dim] // shards_of).reshape((-1,) + (1,) * (len(shape) - 1 - dim))
    return loudness


def centred(own_key, extent, deviation, most, pieces=(), kind=jnp.bfloat16):
    loudness = level_of(own_key, extent, pieces, -0.22, 0.18) if pieces else 1.0
    values = jax.random.normal(own_key, extent, jnp.float32) * deviation * loudness
    return jnp.minimum(jnp.maximum(values, -most), most).astype(kind)


def setup_inputs(seed: int = 0) -> dict:
    splits = jax.random.split(jax.random.key(seed), 4)
    sources = centred(splits[0], (SYSTEMS, NX, NY, NZ), 1.0, 6.0, ((1, 2), (2, 4), (3, 4)), jnp.float32)
    stiffness = jnp.clip(jnp.exp(math.log(2.0) - 1.3862944 * jax.random.uniform(splits[1], (NX, NY, NZ), jnp.float32) ** level_of(splits[1], (NX, NY, NZ), ((0, 2), (1, 4), (2, 4)), -0.2, 0.2)), 0.5, 2.0)
    coarse_inverse = centred(splits[2], (NC, NC), (max(NC // 400, 1)) ** -0.5, 6.0, ((0, 32),), jnp.float32)
    return {"sources": sources, "stiffness": stiffness, "coarse_inverse": coarse_inverse}


damping = 0.8


def loop_sum(padded):
    total = padded[:, 2:, 1:-1, 1:-1] + padded[:, :-2, 1:-1, 1:-1]
    total = total + padded[:, 1:-1, 2:, 1:-1] + padded[:, 1:-1, :-2, 1:-1]
    total = total + padded[:, 1:-1, 1:-1, 2:] + padded[:, 1:-1, 1:-1, :-2]
    return total


def apply_op(answer, weights):
    scaled = weights * answer
    padded = jnp.pad(scaled, ((0, 0), (1, 1), (1, 1), (1, 1)))
    return weights * (6.0 * scaled - loop_sum(padded))


def pre_smooth(source, weights):
    diagonal = 6.0 * weights * weights
    first = damping * source / diagonal
    second = first + damping * (source - apply_op(first, weights)) / diagonal
    return second, source - apply_op(second, weights)


def post_smooth(answer, source, weights):
    return answer + damping * (source - apply_op(answer, weights)) / (6.0 * weights * weights)


def coarsen(values):
    leading = values.shape[0]
    size_x, size_y, size_z = values.shape[1], values.shape[2], values.shape[3]
    blocks = values.reshape((leading, size_x // 2, 2, size_y // 2, 2, size_z // 2, 2))
    return jnp.mean(blocks, axis=(2, 4, 6))


def refine(values):
    return jnp.repeat(jnp.repeat(jnp.repeat(values, 2, axis=1), 2, axis=2), 2, axis=3)


def reference(sources, stiffness, coarse_inverse):
    weight_list = [stiffness[None]]
    for level in range(3):
        weight_list.append(0.5 * coarsen(weight_list[-1]))
    source_list = []
    answer_list = []
    current = sources
    for level in range(4):
        source_list.append(current)
        answer, resid = pre_smooth(current, weight_list[level])
        answer_list.append(answer)
        current = coarsen(resid)
    coarse_source = current
    block_x = CX // 16
    block_y = CY // 16
    block_z = CZ // 16
    ordered = coarse_source.reshape((SYSTEMS, N_GX, block_x, N_GY, block_y, N_GZ, block_z))
    ordered = ordered.transpose((0, 1, 3, 5, 2, 4, 6)).reshape((SYSTEMS, NC))
    solved = jnp.dot(ordered, coarse_inverse.T, precision=lax.Precision.HIGHEST, preferred_element_type=jnp.float32)
    solved = solved.reshape((SYSTEMS, N_GX, N_GY, N_GZ, block_x, block_y, block_z))
    correction = solved.transpose((0, 1, 4, 2, 5, 3, 6)).reshape(coarse_source.shape)
    for level in range(3, -1, -1):
        correction = post_smooth(answer_list[level] + refine(correction), source_list[level], weight_list[level])
    return correction
```

```python
import functools
import jax
import jax.numpy as jnp
from jax import lax
from jax.experimental import pallas as pl
from jax.experimental.pallas import tpu as pltpu
from jax.sharding import PartitionSpec as P

damping = 0.8


def extended(cells, sides, width):
    for axis, dim in sides:
        count = lax.axis_size(axis)
        ends = count - 1
        head = lax.slice_in_dim(cells, 0, width, axis=dim)
        tail = lax.slice_in_dim(cells, cells.shape[dim] - width, cells.shape[dim], axis=dim)
        cells = jnp.concatenate(
            [
                lax.ppermute(tail, axis, [(i, (i + 1) % count) for i in range(ends)]),
                cells,
                lax.ppermute(head, axis, [((i + 1) % count, i) for i in range(ends)]),
            ],
            axis=dim,
        )
    return cells


def loop_sum(padded):
    total = padded[:, 2:, 1:-1, 1:-1] + padded[:, :-2, 1:-1, 1:-1]
    total = total + padded[:, 1:-1, 2:, 1:-1] + padded[:, 1:-1, :-2, 1:-1]
    total = total + padded[:, 1:-1, 1:-1, 2:] + padded[:, 1:-1, 1:-1, :-2]
    return total


def inner_part(values):
    return values[:, 1:-1, 1:-1, 1:-1]


def pre_smooth(source, weights):
    count = source.shape[0]
    stacked = jnp.concatenate([source, weights], axis=0)
    wide = extended(stacked, (("gx", 1), ("gy", 2), ("gz", 3)), 2)
    wide_source = wide[:count]
    wide_weights = wide[count:]
    safe_weights = jnp.where(wide_weights > 0.0, wide_weights, 1.0)
    first = damping * wide_source / (6.0 * safe_weights * safe_weights)
    first_scaled = wide_weights * first
    mid_weights = inner_part(wide_weights)
    mid_safe = inner_part(safe_weights)
    applied = mid_weights * (6.0 * inner_part(first_scaled) - loop_sum(first_scaled))
    second = inner_part(first) + damping * (inner_part(wide_source) - applied) / (
        6.0 * mid_safe * mid_safe
    )
    second_scaled = mid_weights * second
    answer = inner_part(second)
    resid = source - weights * (6.0 * inner_part(second_scaled) - loop_sum(second_scaled))
    return (answer, resid)


def post_smooth(answer, source, weights):
    scaled = weights * answer
    wide = extended(scaled, (("gx", 1), ("gy", 2), ("gz", 3)), 1)
    applied = weights * (6.0 * scaled - loop_sum(wide))
    return answer + damping * (source - applied) / (6.0 * weights * weights)


def coarsen(values):
    leading = values.shape[0]
    size_x, size_y, size_z = (values.shape[1], values.shape[2], values.shape[3])
    blocks = values.reshape((leading, size_x // 2, 2, size_y // 2, 2, size_z // 2, 2))
    return jnp.mean(blocks, axis=(2, 4, 6))


def refine(values):
    return jnp.repeat(jnp.repeat(jnp.repeat(values, 2, axis=1), 2, axis=2), 2, axis=3)


def per_device(sources, stiffness, coarse_inverse):
    weight_list = [stiffness[None]]
    for level in range(3):
        weight_list.append(0.5 * coarsen(weight_list[-1]))
    source_list = []
    answer_list = []
    current = sources
    for level in range(4):
        source_list.append(current)
        answer, resid = pre_smooth(current, weight_list[level])
        answer_list.append(answer)
        current = coarsen(resid)
    count = current.shape[0]
    flat_source = current.reshape((count, -1))
    solved = lax.dot_general(
        lax.all_gather(flat_source, ("gx", "gy", "gz"), axis=1, tiled=True),
        coarse_inverse,
        (((1,), (1,)), ((), ())),
        precision=lax.Precision.HIGHEST,
        preferred_element_type=jnp.float32,
    )
    correction = solved.reshape(current.shape)
    for level in range(3, -1, -1):
        correction = post_smooth(
            answer_list[level] + refine(correction), source_list[level], weight_list[level]
        )
    return correction


K = damping / 6.0
F32 = jnp.float32
BF = jnp.bfloat16


def iota(shape, dim):
    return lax.broadcasted_iota(jnp.int32, shape, dim)


def pick(condition):
    return jnp.where(condition, 1.0, 0.0).astype(BF)


def sel_dot(values, chosen):
    high = values.astype(BF)
    low = (values - high.astype(F32)).astype(BF)
    return jnp.dot(high, chosen, preferred_element_type=F32) + jnp.dot(
        low, chosen, preferred_element_type=F32
    )


def around(c):
    rows, lanes = c.shape
    return (pltpu.roll(c, 1, 0) + pltpu.roll(c, rows - 1, 0)) + (
        pltpu.roll(c, 1, 1) + pltpu.roll(c, lanes - 1, 1)
    )


def whole_sum(planes, nz):
    rows, lanes = planes[0].shape
    row, lane = iota((rows, lanes), 0), iota((rows, lanes), 1)
    outs = []
    for p, c in enumerate(planes):
        s = jnp.where(row > 0, pltpu.roll(c, 1, 0), 0.0) + jnp.where(
            row < rows - 1, pltpu.roll(c, rows - 1, 0), 0.0
        )
        s = s + (
            jnp.where(lane > 0, pltpu.roll(c, 1, 1), 0.0)
            + jnp.where(lane < nz - 1, pltpu.roll(c, lanes - 1, 1), 0.0)
        )
        if p > 0:
            s = s + planes[p - 1]
        if p < len(planes) - 1:
            s = s + planes[p + 1]
        outs.append(s)
    return outs


def kernel(
    dims, b_ref, w_ref, m_ref, f_ref,
    V0, W0, U0, V1, W1, U1, TT, T2, A2, T3, T4, P4, P3, E2, P2, P1,
    SX0, SY0, SZ0, RX0, RY0, RXY0, RZ0,
    SXv, SYv, SZv, RXv, RYv, RXYv, RZv,
    SXw, SYw, SZw, RXw, RYw, RXYw, RZw,
    GM, GW, GB, SW, SB,
    hs, hr, gs, gr,
):
    axes = ("gx", "gy", "gz")
    ix, iy, iz = (lax.axis_index(a) for a in axes)
    n = dims[0] * dims[1] * dims[2]
    me = (ix * dims[1] + iy) * dims[2] + iz

    def place(t):
        return (t // (dims[1] * dims[2]), (t // dims[2]) % dims[1], t % dims[2])

    def other(k):
        return lax.rem(me + k, n)

    barrier = pltpu.get_barrier_semaphore()
    for k in range(1, n):
        pl.semaphore_signal(
            barrier, inc=1, device_id=place(other(k)), device_id_type=pl.DeviceIdType.MESH
        )

    def there(d):
        ok = None
        for i, s, c in zip((ix, iy, iz), dims, d):
            if c:
                t = (i + c < s) if c > 0 else (i + c >= 0)
                ok = t if ok is None else jnp.logical_and(ok, t)
        return ok

    def directions(most):
        found = []
        for dx in (-1, 0, 1):
            for dy in (-1, 0, 1):
                for dz in (-1, 0, 1):
                    if 0 < abs(dx) + abs(dy) + abs(dz) <= most:
                        found.append((dx, dy, dz))
        return found

    def halo_copy(bufs, which, d):
        SX, SY, SZ, RX, RY, RXY, RZ, part = bufs
        dx, dy, dz = d
        up = lambda c: (c + 1) // 2
        down = lambda c: (1 - c) // 2
        if dz:
            s, r = SZ, RZ.at[1 - dx, 1 - dy, down(dz)]
        elif dx and dy:
            rows = SY.shape[2]
            s = SY.at[up(dy), :, pl.ds(rows - part if dx > 0 else 0, part), :]
            r = RXY.at[down(dx), down(dy)]
        elif dx:
            s, r = SX.at[up(dx)], RX.at[down(dx)]
        else:
            s, r = SY.at[up(dy)], RY.at[down(dy)]
        code = ((1 - dx) * 3 + (1 - dy)) * 3 + (1 - dz)
        return pltpu.make_async_remote_copy(
            src_ref=s, dst_ref=r, send_sem=hs.at[which, code], recv_sem=hr.at[which, code],
            device_id=(ix + dx, iy + dy, iz + dz), device_id_type=pl.DeviceIdType.MESH,
        )

    def halo_start(bufs, which, most):
        for d in directions(most):
            @pl.when(there(d))
            def _(d=d):
                halo_copy(bufs, which, d).start()

    def halo_wait(bufs, which, most):
        for d in directions(most):
            back = tuple(-c for c in d)
            @pl.when(there(d))
            def _(back=back):
                halo_copy(bufs, which, back).wait_recv()

    def halo_sent(bufs, which, most):
        for d in directions(most):
            @pl.when(there(d))
            def _(d=d):
                halo_copy(bufs, which, d).wait_send()

    def spread(kind, src, dst, k):
        return pltpu.make_async_remote_copy(
            src_ref=src, dst_ref=dst.at[me], send_sem=gs.at[kind, k], recv_sem=gr.at[kind, me],
            device_id=place(other(k)), device_id_type=pl.DeviceIdType.MESH,
        )

    def arrive(kind, src, dst):
        for k in range(1, n):
            o = other(k)
            pltpu.make_async_remote_copy(
                src_ref=src, dst_ref=dst.at[o], send_sem=gs.at[kind, k], recv_sem=gr.at[kind, o],
                device_id=place(o), device_id_type=pl.DeviceIdType.MESH,
            ).wait_recv()

    nx, ny = b_ref.shape[0], b_ref.shape[1]
    hx, hy = nx // 2, ny // 2
    bufs0 = (SX0, SY0, SZ0, RX0, RY0, RXY0, RZ0, 8)
    bufsv = (SXv, SYv, SZv, RXv, RYv, RXYv, RZv, 16)
    bufsw = (SXw, SYw, SZw, RXw, RYw, RXYw, RZw, 16)

    lane16 = iota((ny, 128), 1)
    packed = jnp.zeros((ny, 128), F32)
    for x in range(nx):
        w = w_ref[x]
        v = K * b_ref[x] / w
        V0[x + 2, 0:ny, 0:128] = v
        W0[x + 2, 0:ny, 0:128] = w
        for a, q in enumerate((v, w)):
            if x < 2:
                SX0[0, a, x] = q
            if x >= nx - 2:
                SX0[1, a, x - nx + 2] = q
            SY0[0, a, 2 * x : 2 * x + 2, :] = q[0:2, :]
            SY0[1, a, 2 * x : 2 * x + 2, :] = q[ny - 2 : ny, :]
            start = 8 * x + 4 * a
            moved = pltpu.roll(q, (start + 2) % 128, 1)
            packed = jnp.where((lane16 >= start) & (lane16 < start + 4), moved, packed)
    SZ0[...] = packed

    pl.semaphore_wait(barrier, n - 1)
    halo_start(bufs0, 0, 2)

    halve = pick(iota((128, 128), 0) == 2 * iota((128, 128), 1))
    halve = halve + pick(iota((128, 128), 0) == 2 * iota((128, 128), 1) + 1)

    def coarsen0(planes):
        for i in range(hx):
            TT[i] = planes(2 * i) + planes(2 * i + 1)
        rows = [
            TT[i, pl.ds(0, hy, stride=2), :] + TT[i, pl.ds(1, hy, stride=2), :] for i in range(hx)
        ]
        return sel_dot(jnp.concatenate(rows, axis=0), halve)

    def coarsen1(planes, SG):
        for i in range(hx // 2):
            T2[pl.ds(8 * i, 8), :] = planes(2 * i) + planes(2 * i + 1)
        for y in range(4):
            A2[pl.ds(4 * y, 4), :] = (
                T2[pl.ds(2 * y, 4, stride=8), :] + T2[pl.ds(2 * y + 1, 4, stride=8), :]
            )
        TT[0] = sel_dot(A2[...], halve)
        total = TT[0, 0:4, :]
        for y in range(1, 4):
            total = total + pltpu.roll(TT[0, 4 * y : 4 * y + 4, :], 32 * y, 1)
        return total

    lane8 = iota((8, 128), 1)

    def pack1(bufs, planes):
        SX, SY, SZ = bufs[:3]
        out = jnp.zeros((8, 128), F32)
        for x in range(hx):
            q = planes[x]
            if x < 3:
                SX[0, 0, x] = q
            if x >= hx - 3:
                SX[1, 0, x - hx + 3] = q
            SY[0, 0, 4 * x : 4 * x + 4, :] = q[0:4, :]
            SY[1, 0, 4 * x : 4 * x + 4, :] = q[4:8, :]
            s = 16 * x
            out = jnp.where((lane8 >= s) & (lane8 < s + 3), pltpu.roll(q, (s - 61) % 128, 1), out)
            out = jnp.where(
                (lane8 >= s + 3) & (lane8 < s + 6), pltpu.roll(q, (s + 3) % 128, 1), out
            )
        SZ[...] = out

    w1 = 0.0625 * coarsen0(lambda x: w_ref[x])
    w1 = [w1[8 * x : 8 * x + 8, :] for x in range(hx)]
    pack1(bufsw, w1)
    halo_start(bufsw, 1, 3)
    SW[...] = 0.0625 * coarsen1(lambda x: w1[x], SW)
    GW[me] = SW[...]
    GM[me] = m_ref[...]
    for k in range(1, n):
        spread(0, SW, GW, k).start()
    for k in range(1, n):
        spread(1, m_ref, GM, k).start()

    def coords(rows, lanes, cy, cz, by, bz):
        r, l = iota((rows, lanes), 0), iota((rows, lanes), 1)
        y = jnp.where(r < cy + (rows - cy) // 2, r, r - rows)
        z = jnp.where(l < cz + (lanes - cz) // 2, l, l - lanes)
        gy, gz = y + iy * cy, z + iz * cz
        ok = (gy >= 0) & (gy < dims[1] * cy) & (gz >= 0) & (gz < dims[2] * cz)
        near = (y >= -by) & (y < cy + by) & (z >= -bz) & (z < cz + bz)
        return jnp.where(ok & near, 1, 0)

    def plane_mask(base, x, cx):
        if 0 <= x < cx:
            return base > 0
        gx = x + ix * cx
        inside = jnp.where((gx >= 0) & (gx < dims[0] * cx), 1, 0)
        return base * inside > 0

    halo_wait(bufs0, 0, 2)
    mask0 = coords(24, 256, ny, 128, 2, 2)
    row8 = iota((8, 128), 0)
    lane24 = iota((24, 128), 1)
    for a, D in ((0, V0), (1, W0)):
        D[0:2, 0:ny, 0:128] = RX0[0, a]
        D[nx + 2 : nx + 4, 0:ny, 0:128] = RX0[1, a]
        for x in range(nx):
            D[x + 2, 16:18, 0:128] = RY0[1, a, 2 * x : 2 * x + 2, :]
            D[x + 2, 22:24, 0:128] = RY0[0, a, 2 * x : 2 * x + 2, :]
        D[1, 16:18, 0:128] = RXY0[0, 1, a, 6:8, :]
        D[1, 22:24, 0:128] = RXY0[0, 0, a, 6:8, :]
        D[nx + 2, 16:18, 0:128] = RXY0[1, 1, a, 0:2, :]
        D[nx + 2, 22:24, 0:128] = RXY0[1, 0, a, 0:2, :]
        for dx in (-1, 0, 1):
            sides = []
            for side in (0, 1):
                mid = RZ0[dx + 1, 1, side]
                if dx == 0:
                    edge = jnp.where(row8 < 4, RZ0[1, 2, side, 0:8, :], RZ0[1, 0, side, 8:16, :])
                else:
                    edge = jnp.zeros((8, 128), F32)
                sides.append(jnp.concatenate([mid, edge], axis=0))
            for x in {-1: (nx - 1,), 0: range(nx), 1: (0,)}[dx]:
                s = 8 * x + 4 * a
                D[x + 2 + dx * nx, :, 128:256] = jnp.where(
                    lane24 < 64,
                    pltpu.roll(sides[1], (-(s + 2)) % 128, 1),
                    pltpu.roll(sides[0], (126 - s) % 128, 1),
                )
        for p in range(nx + 4):
            D[p] = jnp.where(plane_mask(mask0, p - 2, nx), D[p], 0.0)

    for p in range(1, nx + 3):
        c = V0[p]
        u = 1.2 * c + K * (around(c) + (V0[p - 1] + V0[p + 1]))
        U0[p] = jnp.where(plane_mask(mask0, p - 2, nx), u, 0.0)

    def own_sum(ref, p):
        c = ref[p]
        return around(c)[0:ny, 0:128] + (ref[p - 1, 0:ny, 0:128] + ref[p + 1, 0:ny, 0:128])

    def resid0(x):
        p = x + 2
        return b_ref[x] - w_ref[x] * (6.0 * U0[p, 0:ny, 0:128] - own_sum(U0, p))

    b1 = 0.125 * coarsen0(resid0)
    b1 = [b1[8 * x : 8 * x + 8, :] for x in range(hx)]
    v1 = [jnp.where(lane8 < 64, K * b1[x] / jnp.where(lane8 < 64, w1[x], 1.0), 0.0) for x in range(hx)]
    pack1(bufsv, v1)
    halo_start(bufsv, 2, 3)

    mask1 = coords(16, 128, 8, 64, 3, 3)
    lane1 = iota((16, 128), 1)

    def assemble1(bufs, planes, D):
        RX, RY, RXY, RZ = bufs[3:7]
        for dx in (-1, 0, 1):
            sides = []
            for side in (0, 1):
                edge = jnp.where(row8 < 4, RZ[dx + 1, 2, side], RZ[dx + 1, 0, side])
                sides.append(jnp.concatenate([RZ[dx + 1, 1, side], edge], axis=0))
            for x in {-1: range(hx - 3, hx), 0: range(hx), 1: range(3)}[dx]:
                p = x + 3 + dx * hx
                if dx == 0:
                    D[p, 0:8, :] = planes[x]
                    D[p, 8:12, :] = RY[1, 0, 4 * x : 4 * x + 4, :]
                    D[p, 12:16, :] = RY[0, 0, 4 * x : 4 * x + 4, :]
                else:
                    slot = (dx + 1) // 2
                    D[p, 0:8, :] = RX[slot, 0, p if dx < 0 else x]
                    q = 4 * (x - 4 if dx < 0 else x)
                    D[p, 8:12, :] = RXY[slot, 1, 0, q : q + 4, :]
                    D[p, 12:16, :] = RXY[slot, 0, 0, q : q + 4, :]
                s = 16 * x
                ends = jnp.where(
                    lane1 < 96,
                    pltpu.roll(sides[1], (61 - s) % 128, 1),
                    pltpu.roll(sides[0], (125 - s) % 128, 1),
                )
                merged = jnp.where(lane1 < 64, D[p], ends)
                D[p] = jnp.where(plane_mask(mask1, x + dx * hx, hx), merged, 0.0)

    halo_wait(bufsw, 1, 3)
    assemble1(bufsw, w1, W1)

    block = lane8 // 32
    quarter = row8 % 4

    def unpack(G):
        planes = []
        for X in range(4 * dims[0]):
            tiles = []
            for t in range(dims[1] // 2):
                rows = []
                for z in range(dims[2]):
                    d0 = ((X // 4) * dims[1] + 2 * t) * dims[2] + z
                    d1 = d0 + dims[2]
                    q = X % 4
                    rows.append(
                        jnp.where(
                            row8 < 4,
                            jnp.broadcast_to(G[d0, q : q + 1, :], (8, 128)),
                            jnp.broadcast_to(G[d1, q : q + 1, :], (8, 128)),
                        )
                    )
                out = None
                for s in range(4):
                    pre = rows[s % 4]
                    for j in range(1, 4):
                        pre = jnp.where(block == j, rows[(j + s) % 4], pre)
                    moved = pltpu.roll(pre, 32 * s, 1) if s else pre
                    out = moved if out is None else jnp.where(block == (quarter + s) % 4, moved, out)
                tiles.append(out)
            planes.append(jnp.concatenate(tiles, axis=0))
        return planes

    def coarsen2(planes):
        c = len(planes) // 2
        for i in range(c):
            T3[i] = planes[2 * i] + planes[2 * i + 1]
        rows = [T3[i, pl.ds(0, 8, stride=2), :] + T3[i, pl.ds(1, 8, stride=2), :] for i in range(c)]
        out = sel_dot(jnp.concatenate(rows, axis=0), halve)
        return [out[8 * i : 8 * i + 8, :] for i in range(c)]

    arrive(0, SW, GW)
    w2 = unpack(GW)
    w3 = [0.0625 * q for q in coarsen2(w2)]
    valid3 = lane8 < 64
    w3s = [jnp.where(valid3, q, 1.0) for q in w3]

    halo_wait(bufsv, 2, 3)
    assemble1(bufsv, v1, V1)
    for p in range(1, hx + 5):
        c = V1[p]
        u = 1.2 * c + K * (around(c) + (V1[p - 1] + V1[p + 1]))
        U1[p] = jnp.where(plane_mask(mask1, p - 3, hx), u, 0.0)

    def resid1(x):
        p = x + 3
        s = around(U1[p])[0:8, :] + (U1[p - 1, 0:8, :] + U1[p + 1, 0:8, :])
        return jnp.where(lane8 < 64, b1[x] - w1[x] * (6.0 * U1[p, 0:8, :] - s), 0.0)

    SB[...] = 0.125 * coarsen1(resid1, SB)
    GB[me] = SB[...]
    for k in range(1, n):
        spread(2, SB, GB, k).start()
    arrive(1, m_ref, GM)
    arrive(2, SB, GB)

    b2 = unpack(GB)
    v2 = [K * b / w for b, w in zip(b2, w2)]
    u2 = [1.2 * v + K * s for v, s in zip(v2, whole_sum(v2, 128))]
    r2 = [b - w * (6.0 * u - s) for b, w, u, s in zip(b2, w2, u2, whole_sum(u2, 128))]
    b3 = [0.125 * q for q in coarsen2(r2)]
    v3 = [K * b / w for b, w in zip(b3, w3s)]
    u3 = [jnp.where(valid3, 1.2 * v + K * s, 0.0) for v, s in zip(v3, whole_sum(v3, 64))]
    r3 = [b - w * (6.0 * u - s) for b, w, u, s in zip(b3, w3, u3, whole_sum(u3, 64))]
    c4 = len(r3) // 2
    for i in range(c4):
        T4[pl.ds(8 * i, 8), :] = r3[2 * i] + r3[2 * i + 1]
    half = 4 * c4
    b4 = 0.125 * sel_dot(T4[pl.ds(0, half, stride=2), :] + T4[pl.ds(1, half, stride=2), :], halve)
    acc = b4
    for j in range(1, 4):
        acc = jnp.where(quarter == j, pltpu.roll(b4, 32 * j, 1), acc)
    low = jnp.sum(jnp.where(row8 < 4, acc, 0.0), axis=0, keepdims=True)
    high = jnp.sum(jnp.where(row8 >= 4, acc, 0.0), axis=0, keepdims=True)
    cells = GM.shape[0] * GM.shape[1]
    matrix = GM[...].reshape((cells, 256))
    solved = jnp.sum(matrix[:, 0:128] * low + matrix[:, 128:256] * high, axis=1, keepdims=True)
    hit = (iota((cells, 128), 0) % 32) == iota((cells, 128), 1) // 2
    e4 = jnp.sum(jnp.where(hit, solved, 0.0).reshape((cells // 32, 32, 128)), axis=1)
    P4[pl.ds(0, half, stride=2), :] = e4
    P4[pl.ds(1, half, stride=2), :] = e4

    y3 = [u + w * P4[8 * (i // 2) : 8 * (i // 2) + 8, :] for i, (u, w) in enumerate(zip(u3, w3))]
    e3 = [
        jnp.where(valid3, (0.2 * y + v + K * s) / w, 0.0)
        for y, v, s, w in zip(y3, v3, whole_sum(y3, 64), w3s)
    ]
    double = pick(iota((128, 256), 0) == iota((128, 256), 1) // 2)
    wide3 = sel_dot(jnp.concatenate(e3, axis=0), double[:, 0:128])
    for i in range(len(e3)):
        P3[i, pl.ds(0, 8, stride=2), :] = wide3[8 * i : 8 * i + 8, :]
        P3[i, pl.ds(1, 8, stride=2), :] = wide3[8 * i : 8 * i + 8, :]
    y2 = [u + w * P3[i // 2] for i, (u, w) in enumerate(zip(u2, w2))]
    s2 = whole_sum(y2, 128)
    E2[...] = jnp.zeros_like(E2)
    for i in range(len(y2)):
        E2[i + 1, 8:24, :] = (0.2 * y2[i] + v2[i] + K * s2[i]) / w2[i]

    seen = jnp.concatenate([E2[4 * ix + i, pl.ds(6 + 4 * iy, 8), :] for i in range(6)], axis=0)
    j = iota((128, 128), 1)
    zl = jnp.where(j < 96, j // 2, j // 2 - 64) + 32 * iz
    wide2 = sel_dot(seen, pick(iota((128, 128), 0) == zl))
    for i in range(6):
        P2[i, pl.ds(0, 8, stride=2), :] = wide2[8 * i : 8 * i + 8, :]
        P2[i, pl.ds(1, 8, stride=2), :] = wide2[8 * i : 8 * i + 8, :]
    for p in range(1, hx + 5):
        U1[p] = U1[p] + W1[p] * pltpu.roll(P2[(p - 3) // 2 + 1], 12, 0)
    e1 = []
    for p in range(2, hx + 4):
        c = U1[p]
        f = 0.2 * c + V1[p] + K * (around(c) + (U1[p - 1] + U1[p + 1]))
        inside = plane_mask(mask1, p - 3, hx)
        e1.append(jnp.where(inside, f, 0.0) / jnp.where(inside, W1[p], 1.0))
    wide1 = sel_dot(jnp.concatenate(e1, axis=0), double)
    for i in range(hx + 2):
        for t in range(2):
            q = wide1[16 * i : 16 * i + 16, 128 * t : 128 * t + 128]
            P1[t, i, pl.ds(0, 16, stride=2), :] = q
            P1[t, i, pl.ds(1, 16, stride=2), :] = q

    for p in range(1, nx + 3):
        i = (p - 2) // 2 + 1
        parts = []
        for t in range(2):
            edge = jnp.where(row8 < 4, P1[t, i, 16:24, :], P1[t, i, 24:32, :])
            parts.append(jnp.concatenate([P1[t, i, 0:16, :], edge], axis=0))
        U0[p] = U0[p] + W0[p] * jnp.concatenate(parts, axis=1)
    for x in range(nx):
        p = x + 2
        f_ref[x] = 0.2 * U0[p, 0:ny, 0:128] + V0[p, 0:ny, 0:128] + K * own_sum(U0, p)

    halo_sent(bufs0, 0, 2)
    halo_sent(bufsw, 1, 3)
    halo_sent(bufsv, 2, 3)
    for k in range(1, n):
        spread(0, SW, GW, k).wait_send()
        spread(1, m_ref, GM, k).wait_send()
        spread(2, SB, GB, k).wait_send()


def fused(dims, sources, stiffness, coarse_inverse):
    nx, ny, nz = stiffness.shape
    n = dims[0] * dims[1] * dims[2]
    vm = lambda *s: pltpu.VMEM(s, F32)
    halo0 = [
        vm(2, 2, 2, ny, 128), vm(2, 2, 2 * nx, 128), vm(ny, 128),
        vm(2, 2, 2, ny, 128), vm(2, 2, 2 * nx, 128), vm(2, 2, 2, 8, 128), vm(3, 3, 2, ny, 128),
    ]
    halo1 = [
        vm(2, 1, 3, 8, 128), vm(2, 1, 32, 128), vm(8, 128),
        vm(2, 1, 3, 8, 128), vm(2, 1, 32, 128), vm(2, 2, 1, 16, 128), vm(3, 3, 2, 8, 128),
    ]
    scaled = pl.pallas_call(
        functools.partial(kernel, dims),
        out_shape=jax.ShapeDtypeStruct((nx, ny, nz), F32),
        in_specs=[pl.BlockSpec(memory_space=pltpu.VMEM)] * 3,
        out_specs=pl.BlockSpec(memory_space=pltpu.VMEM),
        scratch_shapes=[
            vm(nx + 4, 24, 256), vm(nx + 4, 24, 256), vm(nx + 4, 24, 256),
            vm(14, 16, 128), vm(14, 16, 128), vm(14, 16, 128),
            vm(8, 16, 128), vm(32, 128), vm(16, 128), vm(2 * dims[0], 16, 128),
            vm(16, 128), vm(16, 128), vm(2 * dims[0], 16, 128),
            vm(4 * dims[0] + 2, 32, 128), vm(6, 16, 128), vm(2, 10, 32, 128),
        ]
        + halo0 + halo1 + halo1
        + [
            vm(n, 8, 256), vm(n, 4, 128), vm(n, 4, 128), vm(4, 128), vm(4, 128),
            pltpu.SemaphoreType.DMA((3, 27)), pltpu.SemaphoreType.DMA((3, 27)),
            pltpu.SemaphoreType.DMA((3, n)), pltpu.SemaphoreType.DMA((3, n)),
        ],
        compiler_params=pltpu.CompilerParams(collective_id=0, has_side_effects=True),
        name="cycle",
    )(sources[0], stiffness, coarse_inverse)
    return (scaled / stiffness)[None]


def solution(mesh):
    dims = tuple(mesh.shape[a] for a in ("gx", "gy", "gz"))

    def run(sources, stiffness, coarse_inverse):
        nx, ny, nz = stiffness.shape
        lanes = 128
        cells = coarse_inverse.shape[1]
        levels_fit = (
            sources.shape[0] == 1
            and nx == ny == 16
            and nz == lanes
            and dims[2] * nz == 4 * lanes
            and dims[1] * ny == 64
            and cells == 2 * lanes
        )
        if levels_fit:
            return fused(dims, sources, stiffness, coarse_inverse)
        return per_device(sources, stiffness, coarse_inverse)

    in_specs = (P(None, "gx", "gy", "gz"), P("gx", "gy", "gz"), P(("gx", "gy", "gz"), None))
    out_specs = P(None, "gx", "gy", "gz")
    return jax.shard_map(
        run, mesh=mesh, in_specs=in_specs, out_specs=out_specs, check_vma=False
    )
```

```python
import functools
import jax
import jax.numpy as jnp
from jax import lax
from jax.experimental import pallas as pl
from jax.experimental.pallas import tpu as pltpu
from jax.sharding import PartitionSpec as P

damping = 0.8


def extended(cells, sides, width):
    for axis, dim in sides:
        count = lax.axis_size(axis)
        ends = count - 1
        head = lax.slice_in_dim(cells, 0, width, axis=dim)
        tail = lax.slice_in_dim(cells, cells.shape[dim] - width, cells.shape[dim], axis=dim)
        cells = jnp.concatenate(
            [
                lax.ppermute(tail, axis, [(i, (i + 1) % count) for i in range(ends)]),
                cells,
                lax.ppermute(head, axis, [((i + 1) % count, i) for i in range(ends)]),
            ],
            axis=dim,
        )
    return cells


def loop_sum(padded):
    total = padded[:, 2:, 1:-1, 1:-1] + padded[:, :-2, 1:-1, 1:-1]
    total = total + padded[:, 1:-1, 2:, 1:-1] + padded[:, 1:-1, :-2, 1:-1]
    total = total + padded[:, 1:-1, 1:-1, 2:] + padded[:, 1:-1, 1:-1, :-2]
    return total


def inner_part(values):
    return values[:, 1:-1, 1:-1, 1:-1]


def pre_smooth(source, weights):
    count = source.shape[0]
    stacked = jnp.concatenate([source, weights], axis=0)
    wide = extended(stacked, (("gx", 1), ("gy", 2), ("gz", 3)), 2)
    wide_source = wide[:count]
    wide_weights = wide[count:]
    safe_weights = jnp.where(wide_weights > 0.0, wide_weights, 1.0)
    first = damping * wide_source / (6.0 * safe_weights * safe_weights)
    first_scaled = wide_weights * first
    mid_weights = inner_part(wide_weights)
    mid_safe = inner_part(safe_weights)
    applied = mid_weights * (6.0 * inner_part(first_scaled) - loop_sum(first_scaled))
    second = inner_part(first) + damping * (inner_part(wide_source) - applied) / (
        6.0 * mid_safe * mid_safe
    )
    second_scaled = mid_weights * second
    answer = inner_part(second)
    resid = source - weights * (6.0 * inner_part(second_scaled) - loop_sum(second_scaled))
    return (answer, resid)


def post_smooth(answer, source, weights):
    scaled = weights * answer
    wide = extended(scaled, (("gx", 1), ("gy", 2), ("gz", 3)), 1)
    applied = weights * (6.0 * scaled - loop_sum(wide))
    return answer + damping * (source - applied) / (6.0 * weights * weights)


def coarsen(values):
    leading = values.shape[0]
    size_x, size_y, size_z = (values.shape[1], values.shape[2], values.shape[3])
    blocks = values.reshape((leading, size_x // 2, 2, size_y // 2, 2, size_z // 2, 2))
    return jnp.mean(blocks, axis=(2, 4, 6))


def refine(values):
    return jnp.repeat(jnp.repeat(jnp.repeat(values, 2, axis=1), 2, axis=2), 2, axis=3)


def per_device(sources, stiffness, coarse_inverse):
    weight_list = [stiffness[None]]
    for level in range(3):
        weight_list.append(0.5 * coarsen(weight_list[-1]))
    source_list = []
    answer_list = []
    current = sources
    for level in range(4):
        source_list.append(current)
        answer, resid = pre_smooth(current, weight_list[level])
        answer_list.append(answer)
        current = coarsen(resid)
    count = current.shape[0]
    flat_source = current.reshape((count, -1))
    solved = lax.dot_general(
        lax.all_gather(flat_source, ("gx", "gy", "gz"), axis=1, tiled=True),
        coarse_inverse,
        (((1,), (1,)), ((), ())),
        precision=lax.Precision.HIGHEST,
        preferred_element_type=jnp.float32,
    )
    correction = solved.reshape(current.shape)
    for level in range(3, -1, -1):
        correction = post_smooth(
            answer_list[level] + refine(correction), source_list[level], weight_list[level]
        )
    return correction


K = damping / 6.0
F32 = jnp.float32
BF = jnp.bfloat16


def iota(shape, dim):
    return lax.broadcasted_iota(jnp.int32, shape, dim)


def pick(condition):
    return jnp.where(condition, 1.0, 0.0).astype(BF)


def sel_dot(values, chosen):
    high = values.astype(BF)
    low = (values - high.astype(F32)).astype(BF)
    return jnp.dot(high, chosen, preferred_element_type=F32) + jnp.dot(
        low, chosen, preferred_element_type=F32
    )


def around(c):
    rows, lanes = c.shape
    return (pltpu.roll(c, 1, 0) + pltpu.roll(c, rows - 1, 0)) + (
        pltpu.roll(c, 1, 1) + pltpu.roll(c, lanes - 1, 1)
    )


def whole_sum(planes, nz):
    rows, lanes = planes[0].shape
    row, lane = iota((rows, lanes), 0), iota((rows, lanes), 1)
    outs = []
    for p, c in enumerate(planes):
        s = jnp.where(row > 0, pltpu.roll(c, 1, 0), 0.0) + jnp.where(
            row < rows - 1, pltpu.roll(c, rows - 1, 0), 0.0
        )
        s = s + (
            jnp.where(lane > 0, pltpu.roll(c, 1, 1), 0.0)
            + jnp.where(lane < nz - 1, pltpu.roll(c, lanes - 1, 1), 0.0)
        )
        if p > 0:
            s = s + planes[p - 1]
        if p < len(planes) - 1:
            s = s + planes[p + 1]
        outs.append(s)
    return outs


def kernel(
    dims, b_ref, w_ref, m_ref, f_ref,
    V0, W0, U0, V1, W1, U1, TT, T2, A2, T3, T4, P4, P3, E2, P2, P1,
    SX0, SY0, SZ0, RX0, RY0, RXY0, RZ0,
    SXv, SYv, SZv, RXv, RYv, RXYv, RZv,
    SXw, SYw, SZw, RXw, RYw, RXYw, RZw,
    GM, GW, GB, SW, SB,
    hs, hr, gs, gr,
):
    axes = ("gx", "gy", "gz")
    ix, iy, iz = (lax.axis_index(a) for a in axes)
    n = dims[0] * dims[1] * dims[2]
    me = (ix * dims[1] + iy) * dims[2] + iz

    def place(t):
        return (t // (dims[1] * dims[2]), (t // dims[2]) % dims[1], t % dims[2])

    def other(k):
        return lax.rem(me + k, n)

    barrier = pltpu.get_barrier_semaphore()

    def there(d):
        ok = None
        for i, s, c in zip((ix, iy, iz), dims, d):
            if c:
                t = (i + c < s) if c > 0 else (i + c >= 0)
                ok = t if ok is None else jnp.logical_and(ok, t)
        return ok

    def directions(most):
        found = []
        for dx in (-1, 0, 1):
            for dy in (-1, 0, 1):
                for dz in (-1, 0, 1):
                    if 0 < abs(dx) + abs(dy) + abs(dz) <= most:
                        found.append((dx, dy, dz))
        return found

    for d in directions(3):
        @pl.when(there(d))
        def _(d=d):
            pl.semaphore_signal(
                barrier, inc=1, device_id=(ix + d[0], iy + d[1], iz + d[2]),
                device_id_type=pl.DeviceIdType.MESH,
            )

    def span(i, s):
        return 1 + jnp.where(i > 0, 1, 0) + jnp.where(i < s - 1, 1, 0)

    greeted = span(ix, dims[0]) * span(iy, dims[1]) * span(iz, dims[2]) - 1

    def halo_copy(bufs, which, d):
        SX, SY, SZ, RX, RY, RXY, RZ, part = bufs
        dx, dy, dz = d
        up = lambda c: (c + 1) // 2
        down = lambda c: (1 - c) // 2
        if dz:
            s, r = SZ, RZ.at[1 - dx, 1 - dy, down(dz)]
        elif dx and dy:
            rows = SY.shape[2]
            s = SY.at[up(dy), :, pl.ds(rows - part if dx > 0 else 0, part), :]
            r = RXY.at[down(dx), down(dy)]
        elif dx:
            s, r = SX.at[up(dx)], RX.at[down(dx)]
        else:
            s, r = SY.at[up(dy)], RY.at[down(dy)]
        code = ((1 - dx) * 3 + (1 - dy)) * 3 + (1 - dz)
        return pltpu.make_async_remote_copy(
            src_ref=s, dst_ref=r, send_sem=hs.at[which, code], recv_sem=hr.at[which, code],
            device_id=(ix + dx, iy + dy, iz + dz), device_id_type=pl.DeviceIdType.MESH,
        )

    def halo_start(bufs, which, most):
        for d in directions(most):
            @pl.when(there(d))
            def _(d=d):
                halo_copy(bufs, which, d).start()

    def halo_wait(bufs, which, most):
        for d in directions(most):
            back = tuple(-c for c in d)
            @pl.when(there(d))
            def _(back=back):
                halo_copy(bufs, which, back).wait_recv()

    def halo_sent(bufs, which, most):
        for d in directions(most):
            @pl.when(there(d))
            def _(d=d):
                halo_copy(bufs, which, d).wait_send()

    def spread(kind, src, dst, k):
        return pltpu.make_async_remote_copy(
            src_ref=src, dst_ref=dst.at[me], send_sem=gs.at[kind, k], recv_sem=gr.at[kind, me],
            device_id=place(other(k)), device_id_type=pl.DeviceIdType.MESH,
        )

    def arrive(kind, src, dst):
        for k in range(1, n):
            o = other(k)
            pltpu.make_async_remote_copy(
                src_ref=src, dst_ref=dst.at[o], send_sem=gs.at[kind, k], recv_sem=gr.at[kind, o],
                device_id=place(o), device_id_type=pl.DeviceIdType.MESH,
            ).wait_recv()

    nx, ny = b_ref.shape[0], b_ref.shape[1]
    hx, hy = nx // 2, ny // 2
    bufs0 = (SX0, SY0, SZ0, RX0, RY0, RXY0, RZ0, 8)
    bufsv = (SXv, SYv, SZv, RXv, RYv, RXYv, RZv, 16)
    bufsw = (SXw, SYw, SZw, RXw, RYw, RXYw, RZw, 16)

    lane16 = iota((ny, 128), 1)
    packed = jnp.zeros((ny, 128), F32)
    for x in range(nx):
        w = w_ref[x]
        v = K * b_ref[x] / w
        V0[x + 2, 0:ny, 0:128] = v
        W0[x + 2, 0:ny, 0:128] = w
        for a, q in enumerate((v, w)):
            if x < 2:
                SX0[0, a, x] = q
            if x >= nx - 2:
                SX0[1, a, x - nx + 2] = q
            SY0[0, a, 2 * x : 2 * x + 2, :] = q[0:2, :]
            SY0[1, a, 2 * x : 2 * x + 2, :] = q[ny - 2 : ny, :]
            start = 8 * x + 4 * a
            moved = pltpu.roll(q, (start + 2) % 128, 1)
            packed = jnp.where((lane16 >= start) & (lane16 < start + 4), moved, packed)
    SZ0[...] = packed

    pl.semaphore_wait(barrier, greeted)
    halo_start(bufs0, 0, 2)

    halve = pick(iota((128, 128), 0) == 2 * iota((128, 128), 1))
    halve = halve + pick(iota((128, 128), 0) == 2 * iota((128, 128), 1) + 1)

    def coarsen0(planes):
        for i in range(hx):
            TT[i] = planes(2 * i) + planes(2 * i + 1)
        rows = [
            TT[i, pl.ds(0, hy, stride=2), :] + TT[i, pl.ds(1, hy, stride=2), :] for i in range(hx)
        ]
        return sel_dot(jnp.concatenate(rows, axis=0), halve)

    def coarsen1(planes, SG):
        for i in range(hx // 2):
            T2[pl.ds(8 * i, 8), :] = planes(2 * i) + planes(2 * i + 1)
        for y in range(4):
            A2[pl.ds(4 * y, 4), :] = (
                T2[pl.ds(2 * y, 4, stride=8), :] + T2[pl.ds(2 * y + 1, 4, stride=8), :]
            )
        TT[0] = sel_dot(A2[...], halve)
        total = TT[0, 0:4, :]
        for y in range(1, 4):
            total = total + pltpu.roll(TT[0, 4 * y : 4 * y + 4, :], 32 * y, 1)
        return total

    lane8 = iota((8, 128), 1)

    def pack1(bufs, planes):
        SX, SY, SZ = bufs[:3]
        out = jnp.zeros((8, 128), F32)
        for x in range(hx):
            q = planes[x]
            if x < 3:
                SX[0, 0, x] = q
            if x >= hx - 3:
                SX[1, 0, x - hx + 3] = q
            SY[0, 0, 4 * x : 4 * x + 4, :] = q[0:4, :]
            SY[1, 0, 4 * x : 4 * x + 4, :] = q[4:8, :]
            s = 16 * x
            out = jnp.where((lane8 >= s) & (lane8 < s + 3), pltpu.roll(q, (s - 61) % 128, 1), out)
            out = jnp.where(
                (lane8 >= s + 3) & (lane8 < s + 6), pltpu.roll(q, (s + 3) % 128, 1), out
            )
        SZ[...] = out

    w1 = 0.0625 * coarsen0(lambda x: w_ref[x])
    w1 = [w1[8 * x : 8 * x + 8, :] for x in range(hx)]
    pack1(bufsw, w1)
    SW[...] = 0.0625 * coarsen1(lambda x: w1[x], SW)
    GW[me] = SW[...]
    GM[me] = m_ref[...]

    def coords(rows, lanes, cy, cz, by, bz):
        r, l = iota((rows, lanes), 0), iota((rows, lanes), 1)
        y = jnp.where(r < cy + (rows - cy) // 2, r, r - rows)
        z = jnp.where(l < cz + (lanes - cz) // 2, l, l - lanes)
        gy, gz = y + iy * cy, z + iz * cz
        ok = (gy >= 0) & (gy < dims[1] * cy) & (gz >= 0) & (gz < dims[2] * cz)
        near = (y >= -by) & (y < cy + by) & (z >= -bz) & (z < cz + bz)
        return jnp.where(ok & near, 1, 0)

    def plane_mask(base, x, cx):
        if 0 <= x < cx:
            return base > 0
        gx = x + ix * cx
        inside = jnp.where((gx >= 0) & (gx < dims[0] * cx), 1, 0)
        return base * inside > 0

    halo_wait(bufs0, 0, 2)
    halo_start(bufsw, 1, 3)
    mask0 = coords(24, 256, ny, 128, 2, 2)
    row8 = iota((8, 128), 0)
    lane24 = iota((24, 128), 1)
    for a, D in ((0, V0), (1, W0)):
        D[0:2, 0:ny, 0:128] = RX0[0, a]
        D[nx + 2 : nx + 4, 0:ny, 0:128] = RX0[1, a]
        for x in range(nx):
            D[x + 2, 16:18, 0:128] = RY0[1, a, 2 * x : 2 * x + 2, :]
            D[x + 2, 22:24, 0:128] = RY0[0, a, 2 * x : 2 * x + 2, :]
        D[1, 16:18, 0:128] = RXY0[0, 1, a, 6:8, :]
        D[1, 22:24, 0:128] = RXY0[0, 0, a, 6:8, :]
        D[nx + 2, 16:18, 0:128] = RXY0[1, 1, a, 0:2, :]
        D[nx + 2, 22:24, 0:128] = RXY0[1, 0, a, 0:2, :]
        for dx in (-1, 0, 1):
            sides = []
            for side in (0, 1):
                mid = RZ0[dx + 1, 1, side]
                if dx == 0:
                    edge = jnp.where(row8 < 4, RZ0[1, 2, side, 0:8, :], RZ0[1, 0, side, 8:16, :])
                else:
                    edge = jnp.zeros((8, 128), F32)
                sides.append(jnp.concatenate([mid, edge], axis=0))
            for x in {-1: (nx - 1,), 0: range(nx), 1: (0,)}[dx]:
                s = 8 * x + 4 * a
                D[x + 2 + dx * nx, :, 128:256] = jnp.where(
                    lane24 < 64,
                    pltpu.roll(sides[1], (-(s + 2)) % 128, 1),
                    pltpu.roll(sides[0], (126 - s) % 128, 1),
                )
        for p in range(nx + 4):
            D[p] = jnp.where(plane_mask(mask0, p - 2, nx), D[p], 0.0)

    for p in range(1, nx + 3):
        c = V0[p]
        u = 1.2 * c + K * (around(c) + (V0[p - 1] + V0[p + 1]))
        U0[p] = jnp.where(plane_mask(mask0, p - 2, nx), u, 0.0)

    def own_sum(ref, p):
        c = ref[p]
        return around(c)[0:ny, 0:128] + (ref[p - 1, 0:ny, 0:128] + ref[p + 1, 0:ny, 0:128])

    def resid0(x):
        p = x + 2
        return b_ref[x] - w_ref[x] * (6.0 * U0[p, 0:ny, 0:128] - own_sum(U0, p))

    b1 = 0.125 * coarsen0(resid0)
    b1 = [b1[8 * x : 8 * x + 8, :] for x in range(hx)]
    v1 = [jnp.where(lane8 < 64, K * b1[x] / jnp.where(lane8 < 64, w1[x], 1.0), 0.0) for x in range(hx)]
    pack1(bufsv, v1)
    halo_start(bufsv, 2, 3)

    mask1 = coords(16, 128, 8, 64, 3, 3)
    lane1 = iota((16, 128), 1)

    def assemble1(bufs, planes, D):
        RX, RY, RXY, RZ = bufs[3:7]
        for dx in (-1, 0, 1):
            sides = []
            for side in (0, 1):
                edge = jnp.where(row8 < 4, RZ[dx + 1, 2, side], RZ[dx + 1, 0, side])
                sides.append(jnp.concatenate([RZ[dx + 1, 1, side], edge], axis=0))
            for x in {-1: range(hx - 3, hx), 0: range(hx), 1: range(3)}[dx]:
                p = x + 3 + dx * hx
                if dx == 0:
                    D[p, 0:8, :] = planes[x]
                    D[p, 8:12, :] = RY[1, 0, 4 * x : 4 * x + 4, :]
                    D[p, 12:16, :] = RY[0, 0, 4 * x : 4 * x + 4, :]
                else:
                    slot = (dx + 1) // 2
                    D[p, 0:8, :] = RX[slot, 0, p if dx < 0 else x]
                    q = 4 * (x - 4 if dx < 0 else x)
                    D[p, 8:12, :] = RXY[slot, 1, 0, q : q + 4, :]
                    D[p, 12:16, :] = RXY[slot, 0, 0, q : q + 4, :]
                s = 16 * x
                ends = jnp.where(
                    lane1 < 96,
                    pltpu.roll(sides[1], (61 - s) % 128, 1),
                    pltpu.roll(sides[0], (125 - s) % 128, 1),
                )
                merged = jnp.where(lane1 < 64, D[p], ends)
                D[p] = jnp.where(plane_mask(mask1, x + dx * hx, hx), merged, 0.0)

    halo_wait(bufsw, 1, 3)
    for k in range(1, n):
        spread(0, SW, GW, k).start()
    for k in range(1, n):
        spread(1, m_ref, GM, k).start()
    assemble1(bufsw, w1, W1)

    block = lane8 // 32
    quarter = row8 % 4

    def unpack(G):
        planes = []
        for X in range(4 * dims[0]):
            tiles = []
            for t in range(dims[1] // 2):
                rows = []
                for z in range(dims[2]):
                    d0 = ((X // 4) * dims[1] + 2 * t) * dims[2] + z
                    d1 = d0 + dims[2]
                    q = X % 4
                    rows.append(
                        jnp.where(
                            row8 < 4,
                            jnp.broadcast_to(G[d0, q : q + 1, :], (8, 128)),
                            jnp.broadcast_to(G[d1, q : q + 1, :], (8, 128)),
                        )
                    )
                out = None
                for s in range(4):
                    pre = rows[s % 4]
                    for j in range(1, 4):
                        pre = jnp.where(block == j, rows[(j + s) % 4], pre)
                    moved = pltpu.roll(pre, 32 * s, 1) if s else pre
                    out = moved if out is None else jnp.where(block == (quarter + s) % 4, moved, out)
                tiles.append(out)
            planes.append(jnp.concatenate(tiles, axis=0))
        return planes

    def coarsen2(planes):
        c = len(planes) // 2
        for i in range(c):
            T3[i] = planes[2 * i] + planes[2 * i + 1]
        rows = [T3[i, pl.ds(0, 8, stride=2), :] + T3[i, pl.ds(1, 8, stride=2), :] for i in range(c)]
        out = sel_dot(jnp.concatenate(rows, axis=0), halve)
        return [out[8 * i : 8 * i + 8, :] for i in range(c)]


    halo_wait(bufsv, 2, 3)
    assemble1(bufsv, v1, V1)
    for p in range(1, hx + 5):
        c = V1[p]
        u = 1.2 * c + K * (around(c) + (V1[p - 1] + V1[p + 1]))
        U1[p] = jnp.where(plane_mask(mask1, p - 3, hx), u, 0.0)

    def resid1(x):
        p = x + 3
        s = around(U1[p])[0:8, :] + (U1[p - 1, 0:8, :] + U1[p + 1, 0:8, :])
        return jnp.where(lane8 < 64, b1[x] - w1[x] * (6.0 * U1[p, 0:8, :] - s), 0.0)

    SB[...] = 0.125 * coarsen1(resid1, SB)
    GB[me] = SB[...]
    for k in range(1, n):
        spread(2, SB, GB, k).start()
    arrive(0, SW, GW)
    w2 = unpack(GW)
    w3 = [0.0625 * q for q in coarsen2(w2)]
    valid3 = lane8 < 64
    w3s = [jnp.where(valid3, q, 1.0) for q in w3]
    arrive(2, SB, GB)

    b2 = unpack(GB)
    v2 = [K * b / w for b, w in zip(b2, w2)]
    u2 = [1.2 * v + K * s for v, s in zip(v2, whole_sum(v2, 128))]
    r2 = [b - w * (6.0 * u - s) for b, w, u, s in zip(b2, w2, u2, whole_sum(u2, 128))]
    b3 = [0.125 * q for q in coarsen2(r2)]
    v3 = [K * b / w for b, w in zip(b3, w3s)]
    u3 = [jnp.where(valid3, 1.2 * v + K * s, 0.0) for v, s in zip(v3, whole_sum(v3, 64))]
    r3 = [b - w * (6.0 * u - s) for b, w, u, s in zip(b3, w3, u3, whole_sum(u3, 64))]
    c4 = len(r3) // 2
    for i in range(c4):
        T4[pl.ds(8 * i, 8), :] = r3[2 * i] + r3[2 * i + 1]
    half = 4 * c4
    b4 = 0.125 * sel_dot(T4[pl.ds(0, half, stride=2), :] + T4[pl.ds(1, half, stride=2), :], halve)
    acc = b4
    for j in range(1, 4):
        acc = jnp.where(quarter == j, pltpu.roll(b4, 32 * j, 1), acc)
    low = jnp.sum(jnp.where(row8 < 4, acc, 0.0), axis=0, keepdims=True)
    high = jnp.sum(jnp.where(row8 >= 4, acc, 0.0), axis=0, keepdims=True)
    arrive(1, m_ref, GM)
    cells = GM.shape[0] * GM.shape[1]
    matrix = GM[...].reshape((cells, 256))
    solved = jnp.sum(matrix[:, 0:128] * low + matrix[:, 128:256] * high, axis=1, keepdims=True)
    hit = (iota((cells, 128), 0) % 32) == iota((cells, 128), 1) // 2
    e4 = jnp.sum(jnp.where(hit, solved, 0.0).reshape((cells // 32, 32, 128)), axis=1)
    P4[pl.ds(0, half, stride=2), :] = e4
    P4[pl.ds(1, half, stride=2), :] = e4

    y3 = [u + w * P4[8 * (i // 2) : 8 * (i // 2) + 8, :] for i, (u, w) in enumerate(zip(u3, w3))]
    e3 = [
        jnp.where(valid3, (0.2 * y + v + K * s) / w, 0.0)
        for y, v, s, w in zip(y3, v3, whole_sum(y3, 64), w3s)
    ]
    double = pick(iota((128, 256), 0) == iota((128, 256), 1) // 2)
    wide3 = sel_dot(jnp.concatenate(e3, axis=0), double[:, 0:128])
    for i in range(len(e3)):
        P3[i, pl.ds(0, 8, stride=2), :] = wide3[8 * i : 8 * i + 8, :]
        P3[i, pl.ds(1, 8, stride=2), :] = wide3[8 * i : 8 * i + 8, :]
    y2 = [u + w * P3[i // 2] for i, (u, w) in enumerate(zip(u2, w2))]
    s2 = whole_sum(y2, 128)
    E2[...] = jnp.zeros_like(E2)
    for i in range(len(y2)):
        E2[i + 1, 8:24, :] = (0.2 * y2[i] + v2[i] + K * s2[i]) / w2[i]

    seen = jnp.concatenate([E2[4 * ix + i, pl.ds(6 + 4 * iy, 8), :] for i in range(6)], axis=0)
    j = iota((128, 128), 1)
    zl = jnp.where(j < 96, j // 2, j // 2 - 64) + 32 * iz
    wide2 = sel_dot(seen, pick(iota((128, 128), 0) == zl))
    for i in range(6):
        P2[i, pl.ds(0, 8, stride=2), :] = wide2[8 * i : 8 * i + 8, :]
        P2[i, pl.ds(1, 8, stride=2), :] = wide2[8 * i : 8 * i + 8, :]
    for p in range(1, hx + 5):
        U1[p] = U1[p] + W1[p] * pltpu.roll(P2[(p - 3) // 2 + 1], 12, 0)
    e1 = []
    for p in range(2, hx + 4):
        c = U1[p]
        f = 0.2 * c + V1[p] + K * (around(c) + (U1[p - 1] + U1[p + 1]))
        inside = plane_mask(mask1, p - 3, hx)
        e1.append(jnp.where(inside, f, 0.0) / jnp.where(inside, W1[p], 1.0))
    wide1 = sel_dot(jnp.concatenate(e1, axis=0), double)
    for i in range(hx + 2):
        for t in range(2):
            q = wide1[16 * i : 16 * i + 16, 128 * t : 128 * t + 128]
            P1[t, i, pl.ds(0, 16, stride=2), :] = q
            P1[t, i, pl.ds(1, 16, stride=2), :] = q

    for p in range(1, nx + 3):
        i = (p - 2) // 2 + 1
        parts = []
        for t in range(2):
            edge = jnp.where(row8 < 4, P1[t, i, 16:24, :], P1[t, i, 24:32, :])
            parts.append(jnp.concatenate([P1[t, i, 0:16, :], edge], axis=0))
        U0[p] = U0[p] + W0[p] * jnp.concatenate(parts, axis=1)
    for x in range(nx):
        p = x + 2
        f_ref[x] = 0.2 * U0[p, 0:ny, 0:128] + V0[p, 0:ny, 0:128] + K * own_sum(U0, p)

    halo_sent(bufs0, 0, 2)
    halo_sent(bufsw, 1, 3)
    halo_sent(bufsv, 2, 3)
    for k in range(1, n):
        spread(0, SW, GW, k).wait_send()
        spread(1, m_ref, GM, k).wait_send()
        spread(2, SB, GB, k).wait_send()


def fused(dims, sources, stiffness, coarse_inverse):
    nx, ny, nz = stiffness.shape
    n = dims[0] * dims[1] * dims[2]
    vm = lambda *s: pltpu.VMEM(s, F32)
    halo0 = [
        vm(2, 2, 2, ny, 128), vm(2, 2, 2 * nx, 128), vm(ny, 128),
        vm(2, 2, 2, ny, 128), vm(2, 2, 2 * nx, 128), vm(2, 2, 2, 8, 128), vm(3, 3, 2, ny, 128),
    ]
    halo1 = [
        vm(2, 1, 3, 8, 128), vm(2, 1, 32, 128), vm(8, 128),
        vm(2, 1, 3, 8, 128), vm(2, 1, 32, 128), vm(2, 2, 1, 16, 128), vm(3, 3, 2, 8, 128),
    ]
    scaled = pl.pallas_call(
        functools.partial(kernel, dims),
        out_shape=jax.ShapeDtypeStruct((nx, ny, nz), F32),
        in_specs=[pl.BlockSpec(memory_space=pltpu.VMEM)] * 3,
        out_specs=pl.BlockSpec(memory_space=pltpu.VMEM),
        scratch_shapes=[
            vm(nx + 4, 24, 256), vm(nx + 4, 24, 256), vm(nx + 4, 24, 256),
            vm(14, 16, 128), vm(14, 16, 128), vm(14, 16, 128),
            vm(8, 16, 128), vm(32, 128), vm(16, 128), vm(2 * dims[0], 16, 128),
            vm(16, 128), vm(16, 128), vm(2 * dims[0], 16, 128),
            vm(4 * dims[0] + 2, 32, 128), vm(6, 16, 128), vm(2, 10, 32, 128),
        ]
        + halo0 + halo1 + halo1
        + [
            vm(n, 8, 256), vm(n, 4, 128), vm(n, 4, 128), vm(4, 128), vm(4, 128),
            pltpu.SemaphoreType.DMA((3, 27)), pltpu.SemaphoreType.DMA((3, 27)),
            pltpu.SemaphoreType.DMA((3, n)), pltpu.SemaphoreType.DMA((3, n)),
        ],
        compiler_params=pltpu.CompilerParams(collective_id=0, has_side_effects=True),
        name="cycle",
    )(sources[0], stiffness, coarse_inverse)
    return (scaled / stiffness)[None]


def solution(mesh):
    dims = tuple(mesh.shape[a] for a in ("gx", "gy", "gz"))

    def run(sources, stiffness, coarse_inverse):
        nx, ny, nz = stiffness.shape
        lanes = 128
        cells = coarse_inverse.shape[1]
        levels_fit = (
            sources.shape[0] == 1
            and nx == ny == 16
            and nz == lanes
            and dims[2] * nz == 4 * lanes
            and dims[1] * ny == 64
            and cells == 2 * lanes
        )
        if levels_fit:
            return fused(dims, sources, stiffness, coarse_inverse)
        return per_device(sources, stiffness, coarse_inverse)

    in_specs = (P(None, "gx", "gy", "gz"), P("gx", "gy", "gz"), P(("gx", "gy", "gz"), None))
    out_specs = P(None, "gx", "gy", "gz")
    return jax.shard_map(
        run, mesh=mesh, in_specs=in_specs, out_specs=out_specs, check_vma=False
    )
```

```python
import functools
import jax
import jax.numpy as jnp
from jax import lax
from jax.experimental import pallas as pl
from jax.experimental.pallas import tpu as pltpu
from jax.sharding import PartitionSpec as P

damping = 0.8


def extended(cells, sides, width):
    for axis, dim in sides:
        count = lax.axis_size(axis)
        ends = count - 1
        head = lax.slice_in_dim(cells, 0, width, axis=dim)
        tail = lax.slice_in_dim(cells, cells.shape[dim] - width, cells.shape[dim], axis=dim)
        cells = jnp.concatenate(
            [
                lax.ppermute(tail, axis, [(i, (i + 1) % count) for i in range(ends)]),
                cells,
                lax.ppermute(head, axis, [((i + 1) % count, i) for i in range(ends)]),
            ],
            axis=dim,
        )
    return cells


def loop_sum(padded):
    total = padded[:, 2:, 1:-1, 1:-1] + padded[:, :-2, 1:-1, 1:-1]
    total = total + padded[:, 1:-1, 2:, 1:-1] + padded[:, 1:-1, :-2, 1:-1]
    total = total + padded[:, 1:-1, 1:-1, 2:] + padded[:, 1:-1, 1:-1, :-2]
    return total


def inner_part(values):
    return values[:, 1:-1, 1:-1, 1:-1]


def pre_smooth(source, weights):
    count = source.shape[0]
    stacked = jnp.concatenate([source, weights], axis=0)
    wide = extended(stacked, (("gx", 1), ("gy", 2), ("gz", 3)), 2)
    wide_source = wide[:count]
    wide_weights = wide[count:]
    safe_weights = jnp.where(wide_weights > 0.0, wide_weights, 1.0)
    first = damping * wide_source / (6.0 * safe_weights * safe_weights)
    first_scaled = wide_weights * first
    mid_weights = inner_part(wide_weights)
    mid_safe = inner_part(safe_weights)
    applied = mid_weights * (6.0 * inner_part(first_scaled) - loop_sum(first_scaled))
    second = inner_part(first) + damping * (inner_part(wide_source) - applied) / (
        6.0 * mid_safe * mid_safe
    )
    second_scaled = mid_weights * second
    answer = inner_part(second)
    resid = source - weights * (6.0 * inner_part(second_scaled) - loop_sum(second_scaled))
    return (answer, resid)


def post_smooth(answer, source, weights):
    scaled = weights * answer
    wide = extended(scaled, (("gx", 1), ("gy", 2), ("gz", 3)), 1)
    applied = weights * (6.0 * scaled - loop_sum(wide))
    return answer + damping * (source - applied) / (6.0 * weights * weights)


def coarsen(values):
    leading = values.shape[0]
    size_x, size_y, size_z = (values.shape[1], values.shape[2], values.shape[3])
    blocks = values.reshape((leading, size_x // 2, 2, size_y // 2, 2, size_z // 2, 2))
    return jnp.mean(blocks, axis=(2, 4, 6))


def refine(values):
    return jnp.repeat(jnp.repeat(jnp.repeat(values, 2, axis=1), 2, axis=2), 2, axis=3)


def per_device(sources, stiffness, coarse_inverse):
    weight_list = [stiffness[None]]
    for level in range(3):
        weight_list.append(0.5 * coarsen(weight_list[-1]))
    source_list = []
    answer_list = []
    current = sources
    for level in range(4):
        source_list.append(current)
        answer, resid = pre_smooth(current, weight_list[level])
        answer_list.append(answer)
        current = coarsen(resid)
    count = current.shape[0]
    flat_source = current.reshape((count, -1))
    solved = lax.dot_general(
        lax.all_gather(flat_source, ("gx", "gy", "gz"), axis=1, tiled=True),
        coarse_inverse,
        (((1,), (1,)), ((), ())),
        precision=lax.Precision.HIGHEST,
        preferred_element_type=jnp.float32,
    )
    correction = solved.reshape(current.shape)
    for level in range(3, -1, -1):
        correction = post_smooth(
            answer_list[level] + refine(correction), source_list[level], weight_list[level]
        )
    return correction


K = damping / 6.0
F32 = jnp.float32
BF = jnp.bfloat16


def iota(shape, dim):
    return lax.broadcasted_iota(jnp.int32, shape, dim)


def pick(condition):
    return jnp.where(condition, 1.0, 0.0).astype(BF)


def sel_dot(values, chosen):
    high = values.astype(BF)
    low = (values - high.astype(F32)).astype(BF)
    return jnp.dot(high, chosen, preferred_element_type=F32) + jnp.dot(
        low, chosen, preferred_element_type=F32
    )


def around(c):
    rows, lanes = c.shape
    return (pltpu.roll(c, 1, 0) + pltpu.roll(c, rows - 1, 0)) + (
        pltpu.roll(c, 1, 1) + pltpu.roll(c, lanes - 1, 1)
    )


def whole_sum(planes, nz):
    rows, lanes = planes[0].shape
    row, lane = iota((rows, lanes), 0), iota((rows, lanes), 1)
    outs = []
    for p, c in enumerate(planes):
        s = jnp.where(row > 0, pltpu.roll(c, 1, 0), 0.0) + jnp.where(
            row < rows - 1, pltpu.roll(c, rows - 1, 0), 0.0
        )
        s = s + (
            jnp.where(lane > 0, pltpu.roll(c, 1, 1), 0.0)
            + jnp.where(lane < nz - 1, pltpu.roll(c, lanes - 1, 1), 0.0)
        )
        if p > 0:
            s = s + planes[p - 1]
        if p < len(planes) - 1:
            s = s + planes[p + 1]
        outs.append(s)
    return outs


def kernel(
    dims, b_ref, w_ref, m_ref, f_ref,
    V0, W0, U0, V1, W1, U1, TT, T2, A2, T3, T4, P4, P3, E2, P2, P1,
    SX0, SY0, SZ0, RX0, RY0, RXY0, RZ0,
    SXv, SYv, SZv, RXv, RYv, RXYv, RZv,
    SXw, SYw, SZw, RXw, RYw, RXYw, RZw,
    GM, GW, GB, SW, SB,
    hs, hr, gs, gr, known,
):
    axes = ("gx", "gy", "gz")
    ix, iy, iz = (lax.axis_index(a) for a in axes)
    n = dims[0] * dims[1] * dims[2]
    me = (ix * dims[1] + iy) * dims[2] + iz

    def place(t):
        return (t // (dims[1] * dims[2]), (t // dims[2]) % dims[1], t % dims[2])

    def other(k):
        return lax.rem(me + k, n)

    barrier = pltpu.get_barrier_semaphore()

    def there(d):
        ok = None
        for i, s, c in zip((ix, iy, iz), dims, d):
            if c:
                t = (i + c < s) if c > 0 else (i + c >= 0)
                ok = t if ok is None else jnp.logical_and(ok, t)
        return ok

    def directions(most):
        found = []
        for dx in (-1, 0, 1):
            for dy in (-1, 0, 1):
                for dz in (-1, 0, 1):
                    if 0 < abs(dx) + abs(dy) + abs(dz) <= most:
                        found.append((dx, dy, dz))
        return found

    def greet(sem):
        for d in directions(3):
            @pl.when(there(d))
            def _(d=d):
                pl.semaphore_signal(
                    sem, inc=1, device_id=(ix + d[0], iy + d[1], iz + d[2]),
                    device_id_type=pl.DeviceIdType.MESH,
                )

    greet(barrier)

    def span(i, s):
        return 1 + jnp.where(i > 0, 1, 0) + jnp.where(i < s - 1, 1, 0)

    greeted = span(ix, dims[0]) * span(iy, dims[1]) * span(iz, dims[2]) - 1

    def halo_copy(bufs, which, d):
        SX, SY, SZ, RX, RY, RXY, RZ, part = bufs
        dx, dy, dz = d
        up = lambda c: (c + 1) // 2
        down = lambda c: (1 - c) // 2
        if dz:
            s, r = SZ, RZ.at[1 - dx, 1 - dy, down(dz)]
        elif dx and dy:
            rows = SY.shape[2]
            s = SY.at[up(dy), :, pl.ds(rows - part if dx > 0 else 0, part), :]
            r = RXY.at[down(dx), down(dy)]
        elif dx:
            s, r = SX.at[up(dx)], RX.at[down(dx)]
        else:
            s, r = SY.at[up(dy)], RY.at[down(dy)]
        code = ((1 - dx) * 3 + (1 - dy)) * 3 + (1 - dz)
        return pltpu.make_async_remote_copy(
            src_ref=s, dst_ref=r, send_sem=hs.at[which, code], recv_sem=hr.at[which, code],
            device_id=(ix + dx, iy + dy, iz + dz), device_id_type=pl.DeviceIdType.MESH,
        )

    def halo_start(bufs, which, most):
        for d in directions(most):
            @pl.when(there(d))
            def _(d=d):
                halo_copy(bufs, which, d).start()

    def halo_wait(bufs, which, most):
        for d in directions(most):
            back = tuple(-c for c in d)
            @pl.when(there(d))
            def _(back=back):
                halo_copy(bufs, which, back).wait_recv()

    def halo_sent(bufs, which, most):
        for d in directions(most):
            @pl.when(there(d))
            def _(d=d):
                halo_copy(bufs, which, d).wait_send()

    def spread(kind, src, dst, k):
        return pltpu.make_async_remote_copy(
            src_ref=src, dst_ref=dst.at[me], send_sem=gs.at[kind, k], recv_sem=gr.at[kind, me],
            device_id=place(other(k)), device_id_type=pl.DeviceIdType.MESH,
        )

    def arrive(kind, src, dst):
        for k in range(1, n):
            o = other(k)
            pltpu.make_async_remote_copy(
                src_ref=src, dst_ref=dst.at[o], send_sem=gs.at[kind, k], recv_sem=gr.at[kind, o],
                device_id=place(o), device_id_type=pl.DeviceIdType.MESH,
            ).wait_recv()

    group = n // dims[0]

    def beside(k):
        return ix * group + lax.rem(me - ix * group + k, group)

    def matrix_copy(k, slot):
        return pltpu.make_async_remote_copy(
            src_ref=m_ref, dst_ref=GM.at[slot], send_sem=gs.at[1, k], recv_sem=gr.at[1, slot],
            device_id=place(beside(k)), device_id_type=pl.DeviceIdType.MESH,
        )

    def matrix_half(x):
        half = GM.at[pl.ds(x * group, group)]
        return pltpu.make_async_remote_copy(
            src_ref=half, dst_ref=half, send_sem=gs.at[3, 0], recv_sem=gr.at[3, 0],
            device_id=(1 - ix, iy, iz), device_id_type=pl.DeviceIdType.MESH,
        )

    nx, ny = b_ref.shape[0], b_ref.shape[1]
    hx, hy = nx // 2, ny // 2
    bufs0 = (SX0, SY0, SZ0, RX0, RY0, RXY0, RZ0, 8)
    bufsv = (SXv, SYv, SZv, RXv, RYv, RXYv, RZv, 16)
    bufsw = (SXw, SYw, SZw, RXw, RYw, RXYw, RZw, 16)

    lane16 = iota((ny, 128), 1)
    packed = jnp.zeros((ny, 128), F32)
    for x in range(nx):
        w = w_ref[x]
        v = K * b_ref[x] / w
        V0[x + 2, 0:ny, 0:128] = v
        W0[x + 2, 0:ny, 0:128] = w
        for a, q in enumerate((v, w)):
            if x < 2:
                SX0[0, a, x] = q
            if x >= nx - 2:
                SX0[1, a, x - nx + 2] = q
            SY0[0, a, 2 * x : 2 * x + 2, :] = q[0:2, :]
            SY0[1, a, 2 * x : 2 * x + 2, :] = q[ny - 2 : ny, :]
            start = 8 * x + 4 * a
            moved = pltpu.roll(q, (start + 2) % 128, 1)
            packed = jnp.where((lane16 >= start) & (lane16 < start + 4), moved, packed)
    SZ0[...] = packed

    pl.semaphore_wait(barrier, greeted)
    halo_start(bufs0, 0, 2)
    greet(known.at[0])

    halve = pick(iota((128, 128), 0) == 2 * iota((128, 128), 1))
    halve = halve + pick(iota((128, 128), 0) == 2 * iota((128, 128), 1) + 1)

    def coarsen0(planes):
        for i in range(hx):
            TT[i] = planes(2 * i) + planes(2 * i + 1)
        rows = [
            TT[i, pl.ds(0, hy, stride=2), :] + TT[i, pl.ds(1, hy, stride=2), :] for i in range(hx)
        ]
        return sel_dot(jnp.concatenate(rows, axis=0), halve)

    def coarsen1(planes, SG):
        for i in range(hx // 2):
            T2[pl.ds(8 * i, 8), :] = planes(2 * i) + planes(2 * i + 1)
        for y in range(4):
            A2[pl.ds(4 * y, 4), :] = (
                T2[pl.ds(2 * y, 4, stride=8), :] + T2[pl.ds(2 * y + 1, 4, stride=8), :]
            )
        TT[0] = sel_dot(A2[...], halve)
        total = TT[0, 0:4, :]
        for y in range(1, 4):
            total = total + pltpu.roll(TT[0, 4 * y : 4 * y + 4, :], 32 * y, 1)
        return total

    lane8 = iota((8, 128), 1)

    def pack1(bufs, planes):
        SX, SY, SZ = bufs[:3]
        out = jnp.zeros((8, 128), F32)
        for x in range(hx):
            q = planes[x]
            if x < 3:
                SX[0, 0, x] = q
            if x >= hx - 3:
                SX[1, 0, x - hx + 3] = q
            SY[0, 0, 4 * x : 4 * x + 4, :] = q[0:4, :]
            SY[1, 0, 4 * x : 4 * x + 4, :] = q[4:8, :]
            s = 16 * x
            out = jnp.where((lane8 >= s) & (lane8 < s + 3), pltpu.roll(q, (s - 61) % 128, 1), out)
            out = jnp.where(
                (lane8 >= s + 3) & (lane8 < s + 6), pltpu.roll(q, (s + 3) % 128, 1), out
            )
        SZ[...] = out

    w1 = 0.0625 * coarsen0(lambda x: w_ref[x])
    w1 = [w1[8 * x : 8 * x + 8, :] for x in range(hx)]
    pack1(bufsw, w1)
    SW[...] = 0.0625 * coarsen1(lambda x: w1[x], SW)
    GW[me] = SW[...]
    GM[me] = m_ref[...]
    halo_start(bufsw, 1, 3)
    pl.semaphore_wait(known.at[0], greeted)
    greet(known.at[1])

    def coords(rows, lanes, cy, cz, by, bz):
        r, l = iota((rows, lanes), 0), iota((rows, lanes), 1)
        y = jnp.where(r < cy + (rows - cy) // 2, r, r - rows)
        z = jnp.where(l < cz + (lanes - cz) // 2, l, l - lanes)
        gy, gz = y + iy * cy, z + iz * cz
        ok = (gy >= 0) & (gy < dims[1] * cy) & (gz >= 0) & (gz < dims[2] * cz)
        near = (y >= -by) & (y < cy + by) & (z >= -bz) & (z < cz + bz)
        return jnp.where(ok & near, 1, 0)

    def plane_mask(base, x, cx):
        if 0 <= x < cx:
            return base > 0
        gx = x + ix * cx
        inside = jnp.where((gx >= 0) & (gx < dims[0] * cx), 1, 0)
        return base * inside > 0

    halo_wait(bufs0, 0, 2)
    mask0 = coords(24, 256, ny, 128, 2, 2)
    row8 = iota((8, 128), 0)
    lane24 = iota((24, 128), 1)
    for a, D in ((0, V0), (1, W0)):
        D[0:2, 0:ny, 0:128] = RX0[0, a]
        D[nx + 2 : nx + 4, 0:ny, 0:128] = RX0[1, a]
        for x in range(nx):
            D[x + 2, 16:18, 0:128] = RY0[1, a, 2 * x : 2 * x + 2, :]
            D[x + 2, 22:24, 0:128] = RY0[0, a, 2 * x : 2 * x + 2, :]
        D[1, 16:18, 0:128] = RXY0[0, 1, a, 6:8, :]
        D[1, 22:24, 0:128] = RXY0[0, 0, a, 6:8, :]
        D[nx + 2, 16:18, 0:128] = RXY0[1, 1, a, 0:2, :]
        D[nx + 2, 22:24, 0:128] = RXY0[1, 0, a, 0:2, :]
        for dx in (-1, 0, 1):
            sides = []
            for side in (0, 1):
                mid = RZ0[dx + 1, 1, side]
                if dx == 0:
                    edge = jnp.where(row8 < 4, RZ0[1, 2, side, 0:8, :], RZ0[1, 0, side, 8:16, :])
                else:
                    edge = jnp.zeros((8, 128), F32)
                sides.append(jnp.concatenate([mid, edge], axis=0))
            for x in {-1: (nx - 1,), 0: range(nx), 1: (0,)}[dx]:
                s = 8 * x + 4 * a
                D[x + 2 + dx * nx, :, 128:256] = jnp.where(
                    lane24 < 64,
                    pltpu.roll(sides[1], (-(s + 2)) % 128, 1),
                    pltpu.roll(sides[0], (126 - s) % 128, 1),
                )
        for p in range(nx + 4):
            D[p] = jnp.where(plane_mask(mask0, p - 2, nx), D[p], 0.0)

    for p in range(1, nx + 3):
        c = V0[p]
        u = 1.2 * c + K * (around(c) + (V0[p - 1] + V0[p + 1]))
        U0[p] = jnp.where(plane_mask(mask0, p - 2, nx), u, 0.0)

    def own_sum(ref, p):
        c = ref[p]
        return around(c)[0:ny, 0:128] + (ref[p - 1, 0:ny, 0:128] + ref[p + 1, 0:ny, 0:128])

    def resid0(x):
        p = x + 2
        return b_ref[x] - w_ref[x] * (6.0 * U0[p, 0:ny, 0:128] - own_sum(U0, p))

    b1 = 0.125 * coarsen0(resid0)
    b1 = [b1[8 * x : 8 * x + 8, :] for x in range(hx)]
    v1 = [jnp.where(lane8 < 64, K * b1[x] / jnp.where(lane8 < 64, w1[x], 1.0), 0.0) for x in range(hx)]
    pack1(bufsv, v1)
    halo_start(bufsv, 2, 3)
    pl.semaphore_wait(known.at[1], greeted)
    for k in range(1, n):
        spread(0, SW, GW, k).start()
    for k in range(1, group):
        matrix_copy(k, me).start()

    mask1 = coords(16, 128, 8, 64, 3, 3)
    lane1 = iota((16, 128), 1)

    def assemble1(bufs, planes, D):
        RX, RY, RXY, RZ = bufs[3:7]
        for dx in (-1, 0, 1):
            sides = []
            for side in (0, 1):
                edge = jnp.where(row8 < 4, RZ[dx + 1, 2, side], RZ[dx + 1, 0, side])
                sides.append(jnp.concatenate([RZ[dx + 1, 1, side], edge], axis=0))
            for x in {-1: range(hx - 3, hx), 0: range(hx), 1: range(3)}[dx]:
                p = x + 3 + dx * hx
                if dx == 0:
                    D[p, 0:8, :] = planes[x]
                    D[p, 8:12, :] = RY[1, 0, 4 * x : 4 * x + 4, :]
                    D[p, 12:16, :] = RY[0, 0, 4 * x : 4 * x + 4, :]
                else:
                    slot = (dx + 1) // 2
                    D[p, 0:8, :] = RX[slot, 0, p if dx < 0 else x]
                    q = 4 * (x - 4 if dx < 0 else x)
                    D[p, 8:12, :] = RXY[slot, 1, 0, q : q + 4, :]
                    D[p, 12:16, :] = RXY[slot, 0, 0, q : q + 4, :]
                s = 16 * x
                ends = jnp.where(
                    lane1 < 96,
                    pltpu.roll(sides[1], (61 - s) % 128, 1),
                    pltpu.roll(sides[0], (125 - s) % 128, 1),
                )
                merged = jnp.where(lane1 < 64, D[p], ends)
                D[p] = jnp.where(plane_mask(mask1, x + dx * hx, hx), merged, 0.0)

    halo_wait(bufsw, 1, 3)
    assemble1(bufsw, w1, W1)

    block = lane8 // 32
    quarter = row8 % 4

    def unpack(G):
        planes = []
        for X in range(4 * dims[0]):
            tiles = []
            for t in range(dims[1] // 2):
                rows = []
                for z in range(dims[2]):
                    d0 = ((X // 4) * dims[1] + 2 * t) * dims[2] + z
                    d1 = d0 + dims[2]
                    q = X % 4
                    rows.append(
                        jnp.where(
                            row8 < 4,
                            jnp.broadcast_to(G[d0, q : q + 1, :], (8, 128)),
                            jnp.broadcast_to(G[d1, q : q + 1, :], (8, 128)),
                        )
                    )
                out = None
                for s in range(4):
                    pre = rows[s % 4]
                    for j in range(1, 4):
                        pre = jnp.where(block == j, rows[(j + s) % 4], pre)
                    moved = pltpu.roll(pre, 32 * s, 1) if s else pre
                    out = moved if out is None else jnp.where(block == (quarter + s) % 4, moved, out)
                tiles.append(out)
            planes.append(jnp.concatenate(tiles, axis=0))
        return planes

    def coarsen2(planes):
        c = len(planes) // 2
        for i in range(c):
            T3[i] = planes[2 * i] + planes[2 * i + 1]
        rows = [T3[i, pl.ds(0, 8, stride=2), :] + T3[i, pl.ds(1, 8, stride=2), :] for i in range(c)]
        out = sel_dot(jnp.concatenate(rows, axis=0), halve)
        return [out[8 * i : 8 * i + 8, :] for i in range(c)]


    halo_wait(bufsv, 2, 3)
    assemble1(bufsv, v1, V1)
    for p in range(1, hx + 5):
        c = V1[p]
        u = 1.2 * c + K * (around(c) + (V1[p - 1] + V1[p + 1]))
        U1[p] = jnp.where(plane_mask(mask1, p - 3, hx), u, 0.0)

    def resid1(x):
        p = x + 3
        s = around(U1[p])[0:8, :] + (U1[p - 1, 0:8, :] + U1[p + 1, 0:8, :])
        return jnp.where(lane8 < 64, b1[x] - w1[x] * (6.0 * U1[p, 0:8, :] - s), 0.0)

    SB[...] = 0.125 * coarsen1(resid1, SB)
    GB[me] = SB[...]
    for k in range(1, n):
        spread(2, SB, GB, k).start()
    arrive(0, SW, GW)
    w2 = unpack(GW)
    w3 = [0.0625 * q for q in coarsen2(w2)]
    valid3 = lane8 < 64
    w3s = [jnp.where(valid3, q, 1.0) for q in w3]
    for k in range(1, group):
        matrix_copy(k, beside(k)).wait_recv()
    matrix_half(ix).start()
    arrive(2, SB, GB)

    b2 = unpack(GB)
    v2 = [K * b / w for b, w in zip(b2, w2)]
    u2 = [1.2 * v + K * s for v, s in zip(v2, whole_sum(v2, 128))]
    r2 = [b - w * (6.0 * u - s) for b, w, u, s in zip(b2, w2, u2, whole_sum(u2, 128))]
    b3 = [0.125 * q for q in coarsen2(r2)]
    v3 = [K * b / w for b, w in zip(b3, w3s)]
    u3 = [jnp.where(valid3, 1.2 * v + K * s, 0.0) for v, s in zip(v3, whole_sum(v3, 64))]
    r3 = [b - w * (6.0 * u - s) for b, w, u, s in zip(b3, w3, u3, whole_sum(u3, 64))]
    c4 = len(r3) // 2
    for i in range(c4):
        T4[pl.ds(8 * i, 8), :] = r3[2 * i] + r3[2 * i + 1]
    half = 4 * c4
    b4 = 0.125 * sel_dot(T4[pl.ds(0, half, stride=2), :] + T4[pl.ds(1, half, stride=2), :], halve)
    acc = b4
    for j in range(1, 4):
        acc = jnp.where(quarter == j, pltpu.roll(b4, 32 * j, 1), acc)
    low = jnp.sum(jnp.where(row8 < 4, acc, 0.0), axis=0, keepdims=True)
    high = jnp.sum(jnp.where(row8 >= 4, acc, 0.0), axis=0, keepdims=True)
    matrix_half(1 - ix).wait_recv()
    cells = GM.shape[0] * GM.shape[1]
    matrix = GM[...].reshape((cells, 256))
    solved = jnp.sum(matrix[:, 0:128] * low + matrix[:, 128:256] * high, axis=1, keepdims=True)
    hit = (iota((cells, 128), 0) % 32) == iota((cells, 128), 1) // 2
    e4 = jnp.sum(jnp.where(hit, solved, 0.0).reshape((cells // 32, 32, 128)), axis=1)
    P4[pl.ds(0, half, stride=2), :] = e4
    P4[pl.ds(1, half, stride=2), :] = e4

    y3 = [u + w * P4[8 * (i // 2) : 8 * (i // 2) + 8, :] for i, (u, w) in enumerate(zip(u3, w3))]
    e3 = [
        jnp.where(valid3, (0.2 * y + v + K * s) / w, 0.0)
        for y, v, s, w in zip(y3, v3, whole_sum(y3, 64), w3s)
    ]
    double = pick(iota((128, 256), 0) == iota((128, 256), 1) // 2)
    wide3 = sel_dot(jnp.concatenate(e3, axis=0), double[:, 0:128])
    for i in range(len(e3)):
        P3[i, pl.ds(0, 8, stride=2), :] = wide3[8 * i : 8 * i + 8, :]
        P3[i, pl.ds(1, 8, stride=2), :] = wide3[8 * i : 8 * i + 8, :]
    y2 = [u + w * P3[i // 2] for i, (u, w) in enumerate(zip(u2, w2))]
    s2 = whole_sum(y2, 128)
    E2[...] = jnp.zeros_like(E2)
    for i in range(len(y2)):
        E2[i + 1, 8:24, :] = (0.2 * y2[i] + v2[i] + K * s2[i]) / w2[i]

    seen = jnp.concatenate([E2[4 * ix + i, pl.ds(6 + 4 * iy, 8), :] for i in range(6)], axis=0)
    j = iota((128, 128), 1)
    zl = jnp.where(j < 96, j // 2, j // 2 - 64) + 32 * iz
    wide2 = sel_dot(seen, pick(iota((128, 128), 0) == zl))
    for i in range(6):
        P2[i, pl.ds(0, 8, stride=2), :] = wide2[8 * i : 8 * i + 8, :]
        P2[i, pl.ds(1, 8, stride=2), :] = wide2[8 * i : 8 * i + 8, :]
    for p in range(1, hx + 5):
        U1[p] = U1[p] + W1[p] * pltpu.roll(P2[(p - 3) // 2 + 1], 12, 0)
    e1 = []
    for p in range(2, hx + 4):
        c = U1[p]
        f = 0.2 * c + V1[p] + K * (around(c) + (U1[p - 1] + U1[p + 1]))
        inside = plane_mask(mask1, p - 3, hx)
        e1.append(jnp.where(inside, f, 0.0) / jnp.where(inside, W1[p], 1.0))
    wide1 = sel_dot(jnp.concatenate(e1, axis=0), double)
    for i in range(hx + 2):
        for t in range(2):
            q = wide1[16 * i : 16 * i + 16, 128 * t : 128 * t + 128]
            P1[t, i, pl.ds(0, 16, stride=2), :] = q
            P1[t, i, pl.ds(1, 16, stride=2), :] = q

    for p in range(1, nx + 3):
        i = (p - 2) // 2 + 1
        parts = []
        for t in range(2):
            edge = jnp.where(row8 < 4, P1[t, i, 16:24, :], P1[t, i, 24:32, :])
            parts.append(jnp.concatenate([P1[t, i, 0:16, :], edge], axis=0))
        U0[p] = U0[p] + W0[p] * jnp.concatenate(parts, axis=1)
    for x in range(nx):
        p = x + 2
        f_ref[x] = 0.2 * U0[p, 0:ny, 0:128] + V0[p, 0:ny, 0:128] + K * own_sum(U0, p)

    halo_sent(bufs0, 0, 2)
    halo_sent(bufsw, 1, 3)
    halo_sent(bufsv, 2, 3)
    for k in range(1, n):
        spread(0, SW, GW, k).wait_send()
        spread(2, SB, GB, k).wait_send()
    for k in range(1, group):
        matrix_copy(k, me).wait_send()
    matrix_half(ix).wait_send()


def fused(dims, sources, stiffness, coarse_inverse):
    nx, ny, nz = stiffness.shape
    n = dims[0] * dims[1] * dims[2]
    vm = lambda *s: pltpu.VMEM(s, F32)
    halo0 = [
        vm(2, 2, 2, ny, 128), vm(2, 2, 2 * nx, 128), vm(ny, 128),
        vm(2, 2, 2, ny, 128), vm(2, 2, 2 * nx, 128), vm(2, 2, 2, 8, 128), vm(3, 3, 2, ny, 128),
    ]
    halo1 = [
        vm(2, 1, 3, 8, 128), vm(2, 1, 32, 128), vm(8, 128),
        vm(2, 1, 3, 8, 128), vm(2, 1, 32, 128), vm(2, 2, 1, 16, 128), vm(3, 3, 2, 8, 128),
    ]
    scaled = pl.pallas_call(
        functools.partial(kernel, dims),
        out_shape=jax.ShapeDtypeStruct((nx, ny, nz), F32),
        in_specs=[pl.BlockSpec(memory_space=pltpu.VMEM)] * 3,
        out_specs=pl.BlockSpec(memory_space=pltpu.VMEM),
        scratch_shapes=[
            vm(nx + 4, 24, 256), vm(nx + 4, 24, 256), vm(nx + 4, 24, 256),
            vm(14, 16, 128), vm(14, 16, 128), vm(14, 16, 128),
            vm(8, 16, 128), vm(32, 128), vm(16, 128), vm(2 * dims[0], 16, 128),
            vm(16, 128), vm(16, 128), vm(2 * dims[0], 16, 128),
            vm(4 * dims[0] + 2, 32, 128), vm(6, 16, 128), vm(2, 10, 32, 128),
        ]
        + halo0 + halo1 + halo1
        + [
            vm(n, 8, 256), vm(n, 4, 128), vm(n, 4, 128), vm(4, 128), vm(4, 128),
            pltpu.SemaphoreType.DMA((3, 27)), pltpu.SemaphoreType.DMA((3, 27)),
            pltpu.SemaphoreType.DMA((4, n)), pltpu.SemaphoreType.DMA((4, n)),
            pltpu.SemaphoreType.REGULAR((2,)),
        ],
        compiler_params=pltpu.CompilerParams(collective_id=0, has_side_effects=True),
        name="cycle",
    )(sources[0], stiffness, coarse_inverse)
    return (scaled / stiffness)[None]


def solution(mesh):
    dims = tuple(mesh.shape[a] for a in ("gx", "gy", "gz"))

    def run(sources, stiffness, coarse_inverse):
        nx, ny, nz = stiffness.shape
        lanes = 128
        cells = coarse_inverse.shape[1]
        levels_fit = (
            sources.shape[0] == 1
            and nx == ny == 16
            and nz == lanes
            and dims[2] * nz == 4 * lanes
            and dims[1] * ny == 64
            and cells == 2 * lanes
            and dims[0] == 2
        )
        if levels_fit:
            return fused(dims, sources, stiffness, coarse_inverse)
        return per_device(sources, stiffness, coarse_inverse)

    in_specs = (P(None, "gx", "gy", "gz"), P("gx", "gy", "gz"), P(("gx", "gy", "gz"), None))
    out_specs = P(None, "gx", "gy", "gz")
    return jax.shard_map(
        run, mesh=mesh, in_specs=in_specs, out_specs=out_specs, check_vma=False
    )
```
